32 devices in a mesh: cp: 4 (over z), fsdp: 8 (over y, x, core).
Axes of the slice: x: 2, y: 2, z: 4, core: 2. Of those that a mesh axis runs over, the one named last changes fastest.
Arguments:
- hidden: bfloat16 [128, 512, 2048], P('fsdp', 'cp')
- tok_pos: int32 [128, 512], P('fsdp', 'cp')
- grad_out: bfloat16 [128, 512, 2048], P('fsdp', 'cp')
- norm_gain: float32 [2048], P(('fsdp', 'cp'))
- w_query: bfloat16 [2048, 2048], P(('fsdp', 'cp'))
- w_key: bfloat16 [2048, 256], P(('fsdp', 'cp'))
- w_value: bfloat16 [2048, 256], P(('fsdp', 'cp'))
- w_out: bfloat16 [2048, 2048], P(('fsdp', 'cp'))
Outputs:
- output 1: bfloat16 [128, 512, 2048], P('fsdp', 'cp')
- output 2: bfloat16 [128, 512, 2048], P('fsdp', 'cp')
- output 3: float32 [2048, 2048], P(('fsdp', 'cp'))
- output 4: float32 [2048, 256], P(('fsdp', 'cp'))
- output 5: float32 [2048, 256], P(('fsdp', 'cp'))
- output 6: float32 [2048, 2048], P(('fsdp', 'cp'))
- output 7: float32 [2048], P(('fsdp', 'cp'))
All inputs are finite; a program needn't handle non-finite values.
Results may differ from the reference program's by a relative error of at most 0.00769182.
Values are sent between devices in bfloat16 or wider.
A program may use at most 1 GiB of HBM per device.

```python
import jax
import jax.numpy as jnp
from jax import lax

SEQS_TOTAL = 128
SEQ_LEN = 512
MODEL_DIM = 2048
NUM_HEADS = 16
NUM_KV_HEADS = 2
HEAD_DIM = 128
Q_BLOCK = 32
ROPE_THETA = 1000000.0
RMS_EPS = 1e-5
NEG_BIG = -1e30
SCALE = HEAD_DIM ** -0.5
GROUP_SIZE = NUM_HEADS // NUM_KV_HEADS
N_QBLOCKS = SEQ_LEN // Q_BLOCK


def setup_inputs(seed: int = 0) -> dict:
    rand_keys = jax.random.split(jax.random.key(seed), 8)
    q_cols = NUM_HEADS * HEAD_DIM
    kv_cols = NUM_KV_HEADS * HEAD_DIM
    in_scale = MODEL_DIM ** -0.5
    hidden = jax.random.normal(rand_keys[0], (SEQS_TOTAL, SEQ_LEN, MODEL_DIM), jnp.float32)
    base_pos = jnp.broadcast_to(jnp.arange(SEQ_LEN, dtype=jnp.int32), (SEQS_TOTAL, SEQ_LEN))
    tok_pos = jax.random.permutation(rand_keys[1], base_pos, axis=1, independent=True)
    grad_out = jax.random.normal(rand_keys[2], (SEQS_TOTAL, SEQ_LEN, MODEL_DIM), jnp.float32)
    norm_gain = jax.random.uniform(rand_keys[3], (MODEL_DIM,), jnp.float32, 0.5, 1.5)
    w_query = jax.random.normal(rand_keys[4], (MODEL_DIM, q_cols), jnp.float32) * in_scale
    w_key = jax.random.normal(rand_keys[5], (MODEL_DIM, kv_cols), jnp.float32) * in_scale
    w_value = jax.random.normal(rand_keys[6], (MODEL_DIM, kv_cols), jnp.float32) * in_scale
    w_out = jax.random.normal(rand_keys[7], (q_cols, MODEL_DIM), jnp.float32) * q_cols ** -0.5
    return {'hidden': hidden.astype(jnp.bfloat16), 'tok_pos': tok_pos, 'grad_out': grad_out.astype(jnp.bfloat16), 'norm_gain': norm_gain, 'w_query': w_query.astype(jnp.bfloat16), 'w_key': w_key.astype(jnp.bfloat16), 'w_value': w_value.astype(jnp.bfloat16), 'w_out': w_out.astype(jnp.bfloat16)}


def rope_tables(positions):
    half_dim = HEAD_DIM // 2
    inv_freq = ROPE_THETA ** (-jnp.arange(half_dim, dtype=jnp.float32) / half_dim)
    angles = positions.astype(jnp.float32)[..., None] * inv_freq
    return jnp.cos(angles)[..., None, :], jnp.sin(angles)[..., None, :]


def rope_apply(values, cos_tab, sin_tab):
    half_dim = HEAD_DIM // 2
    first_half = values[..., :half_dim]
    second_half = values[..., half_dim:]
    return jnp.concatenate([first_half * cos_tab - second_half * sin_tab, second_half * cos_tab + first_half * sin_tab], axis=-1)


def rope_transpose(values, cos_tab, sin_tab):
    half_dim = HEAD_DIM // 2
    first_half = values[..., :half_dim]
    second_half = values[..., half_dim:]
    return jnp.concatenate([first_half * cos_tab + second_half * sin_tab, second_half * cos_tab - first_half * sin_tab], axis=-1)


def seq_pass(hidden, tok_pos, grad_out, norm_gain, w_query, w_key, w_value, w_out):
    x_f32 = hidden.astype(jnp.float32)
    inv_rms = lax.rsqrt(jnp.mean(x_f32 * x_f32, axis=-1) + RMS_EPS)
    x_hat = x_f32 * inv_rms[:, None]
    normed = (x_hat * norm_gain).astype(jnp.bfloat16)
    cos_tab, sin_tab = rope_tables(tok_pos)
    q_lin = jnp.dot(normed, w_query, preferred_element_type=jnp.float32).reshape(SEQ_LEN, NUM_HEADS, HEAD_DIM)
    k_lin = jnp.dot(normed, w_key, preferred_element_type=jnp.float32).reshape(SEQ_LEN, NUM_KV_HEADS, HEAD_DIM)
    q_rot = rope_apply(q_lin, cos_tab, sin_tab).astype(jnp.bfloat16)
    k_rot = rope_apply(k_lin, cos_tab, sin_tab).astype(jnp.bfloat16)
    v_val = jnp.dot(normed, w_value, preferred_element_type=jnp.float32).astype(jnp.bfloat16).reshape(SEQ_LEN, NUM_KV_HEADS, HEAD_DIM)
    k_f32 = k_rot.astype(jnp.float32)
    v_f32 = v_val.astype(jnp.float32)
    q_blocks = q_rot.reshape(N_QBLOCKS, Q_BLOCK, NUM_KV_HEADS, GROUP_SIZE, HEAD_DIM)
    pos_blocks = tok_pos.reshape(N_QBLOCKS, Q_BLOCK)

    def block_scores(q_blk, q_pos):
        scores = jnp.einsum('ikgd,jkd->kigj', q_blk.astype(jnp.float32), k_f32) * SCALE
        visible = tok_pos[None, None, None, :] <= q_pos[None, :, None, None]
        return jnp.where(visible, scores, NEG_BIG), visible

    def fwd_block(blk_args):
        q_blk, q_pos = blk_args
        scores, visible = block_scores(q_blk, q_pos)
        row_max = jnp.max(scores, axis=-1)
        att_probs = jnp.where(visible, jnp.exp(scores - row_max[..., None]), 0.0)
        row_sum = jnp.sum(att_probs, axis=-1)
        out_blk = jnp.einsum('kigj,jkd->ikgd', att_probs.astype(jnp.bfloat16).astype(jnp.float32), v_f32)
        out_blk = out_blk / jnp.transpose(row_sum, (1, 0, 2))[..., None]
        return out_blk.astype(jnp.bfloat16), row_max + jnp.log(row_sum)

    attn_out, log_sum = lax.map(fwd_block, (q_blocks, pos_blocks))
    attn_flat = attn_out.reshape(SEQ_LEN, NUM_HEADS * HEAD_DIM)
    result = (x_f32 + jnp.dot(attn_flat, w_out, preferred_element_type=jnp.float32)).astype(jnp.bfloat16)
    grad_w_out = jnp.dot(attn_flat.T, grad_out, preferred_element_type=jnp.float32)
    grad_attn = jnp.dot(grad_out, w_out.T, preferred_element_type=jnp.float32).astype(jnp.bfloat16)
    gout_blocks = grad_attn.reshape(N_QBLOCKS, Q_BLOCK, NUM_KV_HEADS, GROUP_SIZE, HEAD_DIM)
    row_delta = jnp.einsum('nikgd,nikgd->nkig', gout_blocks.astype(jnp.float32), attn_out.astype(jnp.float32))

    def bwd_block(kv_grads, blk_args):
        grad_k, grad_v = kv_grads
        q_blk, q_pos, gout_blk, lse_blk, delta_blk = blk_args
        scores, visible = block_scores(q_blk, q_pos)
        att_probs = jnp.where(visible, jnp.exp(scores - lse_blk[..., None]), 0.0)
        gout_f32 = gout_blk.astype(jnp.float32)
        grad_v = grad_v + jnp.einsum('kigj,ikgd->jkd', att_probs.astype(jnp.bfloat16).astype(jnp.float32), gout_f32)
        grad_probs = jnp.einsum('ikgd,jkd->kigj', gout_f32, v_f32)
        grad_scores = (att_probs * (grad_probs - delta_blk[..., None])).astype(jnp.bfloat16).astype(jnp.float32)
        grad_q = jnp.einsum('kigj,jkd->ikgd', grad_scores, k_f32)
        grad_k = grad_k + jnp.einsum('kigj,ikgd->jkd', grad_scores, q_blk.astype(jnp.float32))
        return (grad_k, grad_v), grad_q

    zero_kv = jnp.zeros((SEQ_LEN, NUM_KV_HEADS, HEAD_DIM), jnp.float32)
    kv_grads, grad_q = lax.scan(bwd_block, (zero_kv, zero_kv), (q_blocks, pos_blocks, gout_blocks, log_sum, row_delta))
    dq_pre = rope_transpose(grad_q.reshape(SEQ_LEN, NUM_HEADS, HEAD_DIM) * SCALE, cos_tab, sin_tab).astype(jnp.bfloat16).reshape(SEQ_LEN, NUM_HEADS * HEAD_DIM)
    dk_pre = rope_transpose(kv_grads[0] * SCALE, cos_tab, sin_tab).astype(jnp.bfloat16).reshape(SEQ_LEN, NUM_KV_HEADS * HEAD_DIM)
    dv_pre = kv_grads[1].astype(jnp.bfloat16).reshape(SEQ_LEN, NUM_KV_HEADS * HEAD_DIM)
    grad_w_query = jnp.dot(normed.T, dq_pre, preferred_element_type=jnp.float32)
    grad_w_key = jnp.dot(normed.T, dk_pre, preferred_element_type=jnp.float32)
    grad_w_value = jnp.dot(normed.T, dv_pre, preferred_element_type=jnp.float32)
    grad_normed = (jnp.dot(dq_pre, w_query.T, preferred_element_type=jnp.float32) + jnp.dot(dk_pre, w_key.T, preferred_element_type=jnp.float32) + jnp.dot(dv_pre, w_value.T, preferred_element_type=jnp.float32))
    grad_xhat = grad_normed * norm_gain
    grad_gain = jnp.sum(grad_normed * x_hat, axis=0)
    grad_x = inv_rms[:, None] * (grad_xhat - x_hat * jnp.mean(grad_xhat * x_hat, axis=-1, keepdims=True))
    grad_hidden = (grad_out.astype(jnp.float32) + grad_x).astype(jnp.bfloat16)
    return result, grad_hidden, (grad_w_query, grad_w_key, grad_w_value, grad_w_out, grad_gain)


def reference(hidden, tok_pos, grad_out, norm_gain, w_query, w_key, w_value, w_out):
    def per_seq(totals, seq_args):
        result, grad_hidden, seq_grads = seq_pass(seq_args[0], seq_args[1], seq_args[2], norm_gain, w_query, w_key, w_value, w_out)
        return jax.tree.map(jnp.add, totals, seq_grads), (result, grad_hidden)

    init_totals = (jnp.zeros(w_query.shape, jnp.float32), jnp.zeros(w_key.shape, jnp.float32), jnp.zeros(w_value.shape, jnp.float32), jnp.zeros(w_out.shape, jnp.float32), jnp.zeros(norm_gain.shape, jnp.float32))
    totals, seq_outs = lax.scan(per_seq, init_totals, (hidden, tok_pos, grad_out))
    return seq_outs[0], seq_outs[1], totals[0], totals[1], totals[2], totals[3], totals[4]
```

```python
import functools

import jax
import jax.numpy as jnp
from jax import lax
from jax.experimental import pallas as pl
from jax.experimental.pallas import tpu as pltpu
from jax.sharding import PartitionSpec as P


HEAD_DIM = 128
HALF = HEAD_DIM // 2
ROPE_THETA = 1000000.0
RMS_EPS = 1e-5
NEG_BIG = -1e30
SCALE = HEAD_DIM ** -0.5
LOG2E = 1.4426950408889634
ALL_AXES = ('fsdp', 'cp')
F32 = jnp.float32
BF16 = jnp.bfloat16
VMEM_LIMIT = 60 * 1024 * 1024


def dot_nn(a, b):
    return lax.dot_general(a, b, (((1,), (0,)), ((), ())), preferred_element_type=F32)


def dot_nt(a, b):
    return lax.dot_general(a, b, (((1,), (1,)), ((), ())), preferred_element_type=F32)


def dot_tn(a, b):
    return lax.dot_general(a, b, (((0,), (0,)), ((), ())), preferred_element_type=F32)


def params():
    return pltpu.CompilerParams(vmem_limit_bytes=VMEM_LIMIT, dimension_semantics=('arbitrary',))


def cost(flops, nbytes):
    return pl.CostEstimate(flops=int(flops), bytes_accessed=int(nbytes), transcendentals=0)


def whole(shape, index=None):
    index = index or (0,) * len(shape)
    return pl.BlockSpec(shape, lambda i: index, pipeline_mode=pl.Buffered(1))


def norm_kv_body(kv_heads, x_ref, gain_ref, wkv_ref, cos_ref, sin_ref, r_ref, *kv_refs):
    x = x_ref[...].astype(F32)
    inv = lax.rsqrt(jnp.mean(x * x, axis=-1, keepdims=True) + RMS_EPS)
    r = (x * inv * gain_ref[...]).astype(BF16)
    r_ref[...] = r
    kv = dot_nn(r, wkv_ref[...])
    cos, sin = cos_ref[...], sin_ref[...]
    for h in range(kv_heads):
        k0 = 2 * h * HEAD_DIM
        a = kv[:, k0:k0 + HEAD_DIM]
        kv_refs[h][...] = (a * cos + pltpu.roll(a, HALF, 1) * sin).astype(BF16)
        kv_refs[kv_heads + h][...] = kv[:, k0 + HEAD_DIM:k0 + 2 * HEAD_DIM].astype(BF16)


def norm_kv(x, gain_row, wkv, cos_rows, sin_rows, kv_heads):
    tokens, width = x.shape
    bm = min(256, tokens)
    rows = lambda w: pl.BlockSpec((bm, w), lambda i: (i, 0))
    head = jax.ShapeDtypeStruct((tokens, HEAD_DIM), BF16)
    return pl.pallas_call(
        functools.partial(norm_kv_body, kv_heads),
        grid=(tokens // bm,),
        in_specs=[rows(width), whole((1, width)), whole(wkv.shape), rows(HEAD_DIM), rows(HEAD_DIM)],
        out_specs=[rows(width)] + [rows(HEAD_DIM)] * (2 * kv_heads),
        out_shape=[jax.ShapeDtypeStruct((tokens, width), BF16)] + [head] * (2 * kv_heads),
        compiler_params=params(),
        cost_estimate=cost(2 * tokens * width * wkv.shape[1] * 2, 4 * tokens * width),
        name='norm_kv',
    )(x, gain_row, wkv, cos_rows, sin_rows)


def q_do_body(heads, r_ref, dy_ref, wq_ref, wo_ref, cos_ref, sin_ref, q_ref, do_ref):
    lin = dot_nn(r_ref[...], wq_ref[...])
    cos, sin = cos_ref[...], sin_ref[...]
    for h in range(heads):
        lanes = slice(h * HEAD_DIM, (h + 1) * HEAD_DIM)
        a = lin[:, lanes]
        q_ref[:, lanes] = (a * cos + pltpu.roll(a, HALF, 1) * sin).astype(BF16)
    do_ref[...] = dot_nt(dy_ref[...], wo_ref[...]).astype(BF16)


def q_do(r, dy, wqo, cos_rows, sin_rows, group, cols):
    tokens, width = r.shape
    bm = min(512, tokens)
    rows = lambda w: pl.BlockSpec((bm, w), lambda i: (i, 0))
    out = jax.ShapeDtypeStruct((tokens, cols), BF16)
    return pl.pallas_call(
        functools.partial(q_do_body, cols // HEAD_DIM),
        grid=(tokens // bm,),
        in_specs=[rows(width), rows(width), whole((width, cols), (0, group)), whole((cols, width), (group, 1)),
                  rows(HEAD_DIM), rows(HEAD_DIM)],
        out_specs=[rows(cols), rows(cols)],
        out_shape=[out, out],
        compiler_params=params(),
        cost_estimate=cost(4 * tokens * width * cols, 8 * tokens * width),
        name='q_do',
    )(r, dy, wqo, wqo, cos_rows, sin_rows)


def attn_body(n_blk, heads, per, q_ref, do_ref, *refs):
    k_refs, v_refs = refs[:n_blk], refs[n_blk:2 * n_blk]
    bias_ref, cos_ref, sin_ref = refs[2 * n_blk:2 * n_blk + 3]
    outs = refs[len(refs) - 2 - 2 * n_blk:]
    o_ref, dq_ref = outs[0], outs[1]
    dk_refs, dv_refs = outs[2:2 + n_blk], outs[2 + n_blk:]
    kc = jnp.concatenate([k[...] for k in k_refs], axis=0)
    vc = jnp.concatenate([v[...] for v in v_refs], axis=0)
    kt, vt = kc.T, vc.T
    bias = jnp.concatenate([bias_ref[0]] * per, axis=1)
    cos = jnp.concatenate([cos_ref[0]] * per, axis=1)
    sin = jnp.concatenate([sin_ref[0]] * per, axis=1)
    q_all, do_all, p_all, ds_all = [], [], [], []
    for c in range(heads // per):
        lanes = [slice((c * per + h) * HEAD_DIM, (c * per + h + 1) * HEAD_DIM) for h in range(per)]
        q = jnp.concatenate([q_ref[:, s] for s in lanes], axis=0)
        do = jnp.concatenate([do_ref[:, s] for s in lanes], axis=0)
        t = dot_nt(kc, q) * (SCALE * LOG2E) + bias
        e = jnp.exp2(t - jnp.max(t, axis=0, keepdims=True))
        inv_l = 1.0 / jnp.sum(e, axis=0, keepdims=True)
        o_t = (dot_nn(vt, e.astype(BF16)) * inv_l).astype(BF16)
        delta = jnp.sum(do.T.astype(F32) * o_t.astype(F32), axis=0, keepdims=True)
        p = e * inv_l
        ds = (p * (dot_nt(vc, do) - delta)).astype(BF16)
        dq_t = dot_nn(kt, ds) * SCALE
        a, b = dq_t[:HALF], dq_t[HALF:]
        dq_t = jnp.concatenate([a * cos + b * sin, b * cos - a * sin], axis=0).astype(BF16)
        o, dq = o_t.T, dq_t.T
        n_rows = o.shape[0] // per
        for h, s in enumerate(lanes):
            o_ref[:, s] = o[h * n_rows:(h + 1) * n_rows]
            dq_ref[:, s] = dq[h * n_rows:(h + 1) * n_rows]
        q_all.append(q)
        do_all.append(do)
        p_all.append(p.astype(BF16))
        ds_all.append(ds)
    dv = dot_nn(jnp.concatenate(p_all, axis=1), jnp.concatenate(do_all, axis=0))
    dk = dot_nn(jnp.concatenate(ds_all, axis=1), jnp.concatenate(q_all, axis=0))
    n_keys = kc.shape[0] // n_blk
    for b in range(n_blk):
        dk_refs[b][...] = dk[b * n_keys:(b + 1) * n_keys]
        dv_refs[b][...] = dv[b * n_keys:(b + 1) * n_keys]


def attention(q, do, ks, vs, bias, cos_t, sin_t, o_prev, group, n_seq, width):
    tokens, cols = q.shape
    rows = tokens // n_seq
    n_blk, heads = len(ks), cols // HEAD_DIM
    per = 2
    blk = pl.BlockSpec((rows, cols), lambda i: (i, 0))
    kv = pl.BlockSpec((rows, HEAD_DIM), lambda i: (i, 0))
    table = pl.BlockSpec((1, HALF, rows), lambda i: (i, 0, 0))
    in_specs = [blk, blk] + [kv] * (2 * n_blk) + [pl.BlockSpec((1, n_blk * rows, rows), lambda i: (i, 0, 0)), table, table]
    args = [q, do, *ks, *vs, bias, cos_t, sin_t]
    aliases = {}
    if o_prev is not None:
        aliases[len(args)] = 0
        in_specs.append(pl.BlockSpec(memory_space=pl.ANY))
        args.append(o_prev)
    part = jax.ShapeDtypeStruct((tokens, HEAD_DIM), F32)
    return pl.pallas_call(
        functools.partial(attn_body, n_blk, heads, per),
        grid=(n_seq,),
        in_specs=in_specs,
        out_specs=[pl.BlockSpec((rows, cols), lambda i: (i, group)), blk] + [kv] * (2 * n_blk),
        out_shape=[jax.ShapeDtypeStruct((tokens, width), BF16), jax.ShapeDtypeStruct((tokens, cols), BF16)]
        + [part] * (2 * n_blk),
        input_output_aliases=aliases,
        compiler_params=params(),
        cost_estimate=cost(24 * tokens * cols * n_blk * rows, 10 * tokens * cols),
        name='attention',
    )(*args)


def out_proj_body(x_ref, o_ref, wo_ref, res_ref):
    res_ref[...] = (x_ref[...].astype(F32) + dot_nn(o_ref[...], wo_ref[...])).astype(BF16)


def out_proj(x, o, wqo):
    tokens, width = x.shape
    bm = min(512, tokens)
    rows = pl.BlockSpec((bm, width), lambda i: (i, 0))
    return pl.pallas_call(
        out_proj_body,
        grid=(tokens // bm,),
        in_specs=[rows, rows, whole((o.shape[1], width), (0, 1))],
        out_specs=rows,
        out_shape=jax.ShapeDtypeStruct((tokens, width), BF16),
        compiler_params=params(),
        cost_estimate=cost(2 * tokens * width * o.shape[1], 8 * tokens * width),
        name='out_proj',
    )(x, o, wqo)


def dr_query_body(n, *refs):
    wq = refs[n][...]
    total = None
    for g in range(n):
        cols = refs[g].shape[1]
        part = dot_nt(refs[g][...], wq[:, g * cols:(g + 1) * cols])
        total = part if total is None else total + part
    refs[n + 1][...] = total


def dr_query(dqs, wqo):
    tokens, cols = dqs[0].shape
    width = wqo.shape[0]
    bm = min(256, tokens)
    rows = lambda w: pl.BlockSpec((bm, w), lambda i: (i, 0))
    return pl.pallas_call(
        functools.partial(dr_query_body, len(dqs)),
        grid=(tokens // bm,),
        in_specs=[rows(cols)] * len(dqs) + [whole((width, cols * len(dqs)))],
        out_specs=rows(width),
        out_shape=jax.ShapeDtypeStruct((tokens, width), F32),
        compiler_params=params(),
        cost_estimate=cost(2 * tokens * width * cols * len(dqs), 8 * tokens * width),
        name='dr_query',
    )(*dqs, wqo)


def norm_back_body(x_ref, dy_ref, dr_ref, dkv0_ref, dkv1_ref, wkv_ref, gain_ref, gh_ref, gg_ref):
    x = x_ref[...].astype(F32)
    inv = lax.rsqrt(jnp.mean(x * x, axis=-1, keepdims=True) + RMS_EPS)
    n = x * inv
    dr = dr_ref[...] + dot_nt(jnp.concatenate([dkv0_ref[...], dkv1_ref[...]], axis=1), wkv_ref[...])
    prod = dr * n
    part = jnp.sum(prod.reshape(prod.shape[0] // 8, 8, prod.shape[1]), axis=0)

    @pl.when(pl.program_id(0) == 0)
    def _():
        gg_ref[...] = part

    @pl.when(pl.program_id(0) > 0)
    def _():
        gg_ref[...] = gg_ref[...] + part

    gain = gain_ref[...]
    mean = jnp.mean(prod * gain, axis=-1, keepdims=True)
    gh_ref[...] = (dy_ref[...].astype(F32) + inv * (dr * gain - n * mean)).astype(BF16)


def norm_back(x, dy, dr, dkvs, wkv, gain_row):
    tokens, width = x.shape
    bm = min(256, tokens)
    rows = lambda w: pl.BlockSpec((bm, w), lambda i: (i, 0))
    return pl.pallas_call(
        norm_back_body,
        grid=(tokens // bm,),
        in_specs=[rows(width)] * 3 + [rows(2 * HEAD_DIM)] * 2 + [whole(wkv.shape), whole((1, width))],
        out_specs=[rows(width), pl.BlockSpec((8, width), lambda i: (0, 0))],
        out_shape=[jax.ShapeDtypeStruct((tokens, width), BF16), jax.ShapeDtypeStruct((8, width), F32)],
        compiler_params=params(),
        cost_estimate=cost(4 * tokens * width * wkv.shape[1], 14 * tokens * width),
        name='norm_back',
    )(x, dy, dr, *dkvs, wkv, gain_row)


def solution(mesh):
    cp_size, fsdp_size = mesh.shape['cp'], mesh.shape['fsdp']

    def shift(values, step):
        return lax.ppermute(values, 'cp', [(i, (i + step) % cp_size) for i in range(cp_size)])

    def swap(values, axis, bit):
        return lax.ppermute(values, axis, [(i, i ^ bit) for i in range(mesh.shape[axis])])

    def bit_set(axis, bit):
        return (lax.axis_index(axis) & bit) != 0

    def after(values, gate):
        return lax.optimization_barrier((tuple(values), tuple(gate)))[0]

    def gather_small(shard):
        def join(own, axis, bit, at):
            other = swap(own, axis, bit)
            upper = bit_set(axis, bit)
            return jnp.stack([jnp.where(upper, other, own), jnp.where(upper, own, other)], axis=at)

        full = join(shard, 'cp', 1, 0)
        full = join(full, 'cp', 2, 0)
        full = full.reshape((cp_size,) + shard.shape)
        full = join(full, 'fsdp', 4, 0)
        full = join(full, 'fsdp', 2, 1)
        full = join(full, 'fsdp', 1, 2)
        return full.reshape((fsdp_size * cp_size * shard.shape[0],) + shard.shape[1:])

    def scatter_small(total):
        part = total
        for axis, bits in (('fsdp', (4, 2, 1)), ('cp', (2, 1))):
            for bit in bits:
                half = part.shape[0] // 2
                upper = bit_set(axis, bit)
                low, high = part[:half], part[half:]
                part = jnp.where(upper, high, low) + swap(jnp.where(upper, low, high), axis, bit)
        return part

    def scatter_fsdp(part_sum):
        return lax.psum_scatter(part_sum, 'fsdp', scatter_dimension=0, tiled=True)

    def scatter_cp(part_sum):
        return lax.psum_scatter(part_sum, 'cp', scatter_dimension=0, tiled=True)

    def block(hidden, tok_pos, grad_out, norm_gain, w_query, w_key, w_value, w_out):
        n_seq, n_rows, width = hidden.shape
        tokens = n_seq * n_rows
        q_cols, kv_cols = w_query.shape[1], w_key.shape[1]
        kv_heads = kv_cols // HEAD_DIM
        cols = q_cols // kv_heads
        x = hidden.reshape(tokens, width)
        dy = grad_out.reshape(tokens, width)

        wqo = lax.all_gather(jnp.concatenate([w_query, w_out], axis=1), ALL_AXES, axis=0, tiled=True)
        gain_row = gather_small(norm_gain).reshape(1, width)
        wkv = gather_small(jnp.concatenate([w_key[:, :HEAD_DIM], w_value[:, :HEAD_DIM], w_key[:, HEAD_DIM:], w_value[:, HEAD_DIM:]], axis=1))

        inv_freq = ROPE_THETA ** (-jnp.arange(HALF, dtype=F32) / HALF)
        pos_f = tok_pos.astype(F32)
        angles = pos_f.reshape(tokens, 1) * inv_freq
        cos, sin = jnp.cos(angles), jnp.sin(angles)
        cos_rows = jnp.concatenate([cos, cos], axis=1)
        sin_rows = jnp.concatenate([-sin, sin], axis=1)
        angles_t = pos_f[:, None, :] * inv_freq[None, :, None]
        cos_t, sin_t = jnp.cos(angles_t), jnp.sin(angles_t)
        key_pos = jnp.concatenate([tok_pos] + [shift(tok_pos, d) for d in range(1, cp_size)], axis=1)
        bias = jnp.where(key_pos[:, :, None] <= tok_pos[:, None, :], 0.0, NEG_BIG).astype(F32)

        r, *kv = norm_kv(x, gain_row, wkv, cos_rows, sin_rows, kv_heads)

        keys, values, gate = [], [], ()
        for g in range(kv_heads):
            k, v = after((kv[g], kv[kv_heads + g]), gate)
            ks, vs = [k], [v]
            for _ in range(cp_size - 1):
                gate = (ks[-1], vs[-1])
                ks.append(shift(ks[-1], 1))
                vs.append(shift(vs[-1], -1))
            keys.append(ks)
            values.append([vs[0]] + vs[:0:-1])

        def ring_step(s, sums, parts, gate):
            moved = shift(sums[0], 1), shift(sums[1], -1)
            dk, dv = after(moved, gate)
            b = s + 1
            return dk + parts[b % cp_size], dv + parts[cp_size + (cp_size - b) % cp_size]

        def attend(g, o):
            q, do = q_do(r, dy, wqo, cos_rows, sin_rows, g, cols)
            o, dq, *parts = attention(q, do, keys[g], values[g], bias, cos_t, sin_t, o, g, n_seq, q_cols)
            return o, dq, parts, (parts[1], parts[2 * cp_size - 1])

        o, dq0, parts0, sums0 = attend(0, None)
        o, dq1, parts1, sums1 = attend(1, o)
        sums0 = ring_step(1, sums0, parts0, (dq1,))
        part_wo = dot_tn(o, dy)
        half_wo = scatter_fsdp(part_wo)
        part_wq0 = dot_tn(r, dq0)
        half_wq0 = scatter_fsdp(part_wq0)
        part_wq1 = dot_tn(r, dq1)
        half_wq1 = scatter_fsdp(part_wq1)
        sums0 = ring_step(2, sums0, parts0, (part_wo, part_wq0, part_wq1))
        sums1 = ring_step(1, sums1, parts1, (part_wo, part_wq0, part_wq1))
        dr = dr_query((dq0, dq1), wqo)
        result = out_proj(x, o, wqo)
        sums0 = ring_step(3, sums0, parts0, (dr,))
        sums1 = ring_step(2, sums1, parts1, (dr, result))

        def pair_back(sums):
            a = sums[0] * SCALE
            dk = a * cos_rows - jnp.concatenate([a[:, HALF:], a[:, :HALF]], axis=1) * sin_rows
            return jnp.concatenate([dk, sums[1]], axis=1).astype(BF16)

        dkv0 = pair_back(sums0)
        part_wkv0 = dot_tn(r, dkv0)
        half_wkv0 = scatter_fsdp(after((part_wkv0,), (half_wq0, half_wq1))[0])
        grad_wo, grad_wq0, grad_wq1 = scatter_cp(half_wo), scatter_cp(half_wq0), scatter_cp(half_wq1)
        sums1 = ring_step(3, sums1, parts1, (part_wkv0,))
        dkv1 = pair_back(sums1)
        part_wkv1 = dot_tn(r, dkv1)
        half_wkv1 = scatter_fsdp(after((part_wkv1,), (grad_wo, grad_wq0, grad_wq1, half_wkv0))[0])
        grad_wkv0, grad_wkv1 = scatter_cp(half_wkv0), scatter_cp(half_wkv1)
        grad_hidden, gain_parts = norm_back(x, dy, dr, (dkv0, dkv1), wkv, gain_row)
        grad_gain = scatter_small(jnp.sum(gain_parts, axis=0))
        grad_wk = jnp.concatenate([grad_wkv0[:, :HEAD_DIM], grad_wkv1[:, :HEAD_DIM]], axis=1)
        grad_wv = jnp.concatenate([grad_wkv0[:, HEAD_DIM:], grad_wkv1[:, HEAD_DIM:]], axis=1)
        grad_wq = jnp.concatenate([grad_wq0, grad_wq1], axis=1)
        return (result.reshape(hidden.shape), grad_hidden.reshape(hidden.shape), grad_wq, grad_wk, grad_wv,
                grad_wo, grad_gain)

    row_spec = P('fsdp', 'cp', None)
    pos_spec = P('fsdp', 'cp')
    weight_spec = P(ALL_AXES, None)
    gain_spec = P(ALL_AXES)
    return jax.shard_map(block, mesh=mesh, in_specs=(row_spec, pos_spec, row_spec, gain_spec, weight_spec, weight_spec, weight_spec, weight_spec), out_specs=(row_spec, row_spec, weight_spec, weight_spec, weight_spec, weight_spec, gain_spec), check_vma=False)
```
